256 devices in a mesh: lon: 64 (over y, x_lo, z), lat: 4 (over x_hi, core).
Axes of the slice: x: 4 (x_hi: 2, x_lo: 2; x = x_hi * 2 + x_lo), y: 4, z: 8, core: 2. Of those that a mesh axis runs over, the one named last changes fastest.
Arguments:
- perturbation: float32 [80, 1024, 4096], P(None, 'lon', 'lat'), may hold values from -6 to 6
- weight_table: float32 [8, 2048], P(None, 'lat'), may hold values from 0.1 to 1
- band_index: int32 [13], replicated, may hold values from 0 to 7
Outputs:
- localized: float32 [80, 1024, 4096], P(None, 'lon', 'lat')
The draws below stay inside these ranges and needn't reach their ends.
Inputs may be any that keep to these rules, and one draw needn't show every extreme that they name: `band_index`: each entry names a row of weight_table.
All inputs are finite; a program needn't handle non-finite values.
Results may differ from the reference program's by a relative error of at most 0.00005.
Values sent between devices are 32-bit elements; how exact they have to be, the bound alone decides.
A program may use at most 128 MiB of HBM per device.

```python
import math
import jax
import jax.numpy as jnp
from jax import lax

MEMBERS = 80
LEVELS = 4
TABLE = 8
BANDS = 13
NLON = 1024
NLAT = 4096


def touch_ends(drawn, own_key, smallest, largest):
    longest = drawn.shape.index(max(drawn.shape))
    spots = []
    for shift in (0, 1):
        where = [jax.random.randint(jax.random.fold_in(own_key, axis), (), 0, length) for axis, length in enumerate(drawn.shape)]
        where[longest] = (where[longest] + shift) % drawn.shape[longest]
        spots.append(tuple(where))
    return drawn.at[spots[0]].set(smallest).at[spots[1]].set(largest)


def levels(key, shape, pieces, low, largest):
    loudness, own = 1.0, jax.random.fold_in(key, 6)
    for axis_at, shards_of in pieces:
        draws = jnp.exp(jax.random.uniform(jax.random.fold_in(own, axis_at), (shards_of,), jnp.float32, low / len(pieces), largest / len(pieces)))
        loudness = loudness * jnp.repeat(draws, shape[axis_at] // shards_of).reshape([-1 if axis == axis_at else 1 for axis in range(len(shape))])
    return loudness


def noise(rng, shape, deviation, bound, shards=(), dtype=jnp.bfloat16):
    loudness = levels(rng, shape, shards, -0.22, 0.18) if shards else 1.0
    array = jax.random.normal(rng, shape, jnp.float32) * deviation * loudness
    return jnp.minimum(jnp.maximum(array, -bound), bound).astype(dtype)


def setup_inputs(seed: int = 0) -> dict:
    keys = jax.random.split(jax.random.key(seed), 4)
    return {
        "perturbation": noise(keys[0], (MEMBERS, NLON, NLAT), 1.0, 6.0, ((1, 64), (2, 4)), jnp.float32),
        "weight_table": jnp.clip(jnp.exp(math.log(1.0) - 2.3025851 * jax.random.uniform(keys[1], (TABLE, NLAT // 2), jnp.float32) ** levels(keys[1], (TABLE, NLAT // 2), ((1, 4),), -0.2, 0.2)), 0.1, 1.0),
        "band_index": touch_ends(jax.random.randint(keys[2], (BANDS,), 0, TABLE), jax.random.fold_in(keys[2], 1), 0, TABLE - 1).astype(jnp.int32),
    }


root_three = math.sqrt(3.0)
low_taps = [(1.0 + root_three) / (4.0 * math.sqrt(2.0)), (3.0 + root_three) / (4.0 * math.sqrt(2.0)), (3.0 - root_three) / (4.0 * math.sqrt(2.0)), (1.0 - root_three) / (4.0 * math.sqrt(2.0))]
high_taps = [low_taps[3], -low_taps[2], low_taps[1], -low_taps[0]]

def analyze(extended, count, axis, taps):
    result = taps[0] * lax.slice_in_dim(extended, 0, count - 1, 2, axis)
    for tap in range(1, 4):
        result = result + taps[tap] * lax.slice_in_dim(extended, tap, tap + count - 1, 2, axis)
    return result

def synthesize(low, high, prev_low, prev_high, axis):
    even = low_taps[0] * low + low_taps[2] * prev_low + high_taps[0] * high + high_taps[2] * prev_high
    odd = low_taps[1] * low + low_taps[3] * prev_low + high_taps[1] * high + high_taps[3] * prev_high
    paired = jnp.stack([even, odd], axis + 1)
    shape = list(low.shape)
    shape[axis] = shape[axis] * 2
    return paired.reshape(shape)

def profile(weight_table, entry, level):
    return weight_table[entry][::2 ** level][None, None, :]

def lat_split(field):
    extended = jnp.concatenate([field, jnp.zeros(field.shape[:2] + (2,), jnp.float32)], 2)
    count = field.shape[2]
    return (analyze(extended, count, 2, low_taps), analyze(extended, count, 2, high_taps))

def lat_join(low, high):
    zeros = jnp.zeros(low.shape[:2] + (1,), jnp.float32)
    prev_low = jnp.concatenate([zeros, low[:, :, :-1]], 2)
    prev_high = jnp.concatenate([zeros, high[:, :, :-1]], 2)
    return synthesize(low, high, prev_low, prev_high, 2)

def reference(perturbation, weight_table, band_index):
    current = perturbation
    details = []
    for level in range(LEVELS):
        count = current.shape[1]
        extended = jnp.concatenate([current, current[:, :2]], 1)
        lon_low = analyze(extended, count, 1, low_taps)
        lon_high = analyze(extended, count, 1, high_taps)
        coarse, band_zero = lat_split(lon_low)
        band_one, band_two = lat_split(lon_high)
        bands = [band_zero, band_one, band_two]
        details.append([bands[b] * profile(weight_table, band_index[3 * level + b], level) for b in range(3)])
        current = coarse
    current = current * profile(weight_table, band_index[3 * LEVELS], LEVELS - 1)
    for level in reversed(range(LEVELS)):
        bands = details[level]
        lon_low = lat_join(current, bands[0])
        lon_high = lat_join(bands[1], bands[2])
        current = synthesize(lon_low, lon_high, jnp.roll(lon_low, 1, 1), jnp.roll(lon_high, 1, 1), 1)
    return current
```

```python
import math

import jax
import jax.numpy as jnp
from jax import lax
from jax.experimental import pallas as pl
from jax.experimental.pallas import tpu as pltpu
from jax.sharding import PartitionSpec as P

F32 = jnp.float32
LANES = 128
M = 16
LON = 16
HALO = 32
Q = math.sqrt(3.0)
R = 2.0 - Q
H0 = (1.0 + Q) / (4.0 * math.sqrt(2.0))
MESH = pl.DeviceIdType.MESH
MAIN = (8, 4, 2, 1)
USED = (2 * HALO, HALO, HALO // 2, HALO // 4)
OFFSETS = (0, 2, 4, 6, 8, 10)

GATHER = lax.GatherDimensionNumbers(
    offset_dims=(),
    collapsed_slice_dims=(1,),
    start_index_map=(1,),
    operand_batching_dims=(0,),
    start_indices_batching_dims=(0,),
)


def lane_ids(rows):
    return lax.broadcasted_iota(jnp.int32, (rows, LANES), 1)


def permute(x, index):
    return lax.gather(
        x, index[..., None], GATHER, (1, 1), mode=lax.GatherScatterMode.PROMISE_IN_BOUNDS
    )


def roll(x, by):
    by = by % LANES
    return x if by == 0 else pltpu.roll(x, by, 1)


def patterns(rows):
    lane = lane_ids(rows)
    front = lane < 64
    half = lane & 63
    even_odd = 2 * half + jnp.where(front, 0, 1)
    odd_even = 2 * half + jnp.where(front, 1, 0)
    pair = lane >> 1
    odd = lane & 1
    join_front = pair + 64 * odd
    join_back = pair + 64 - 64 * odd
    return lane, front, even_odd, odd_even, join_front, join_back


def split_pair(a, b, pat):
    _, front, even_odd, odd_even, _, _ = pat
    pa = permute(a, even_odd)
    if b is None:
        return pa, roll(pa, 64)
    pb = permute(b, odd_even)
    return jnp.where(front, pa, pb), roll(jnp.where(front, pb, pa), 64)


def join_pair(even, odd, pat, both=True):
    _, front, _, _, join_front, join_back = pat
    turned = roll(odd, 64)
    a = permute(jnp.where(front, even, turned), join_front)
    if not both:
        return [a]
    return [a, permute(jnp.where(front, turned, even), join_back)]


def shift_left(tiles, used, pat):
    lane = pat[0]
    if len(tiles) == 1:
        t = tiles[0]
        last = 64 + used - 1
        return [jnp.where(lane == last, roll(t, last), roll(t, -1))]
    turned = [roll(t, -1) for t in tiles]
    shifted = [
        jnp.where(lane == LANES - 1, turned[b + 1], turned[b]) for b in range(len(tiles) - 1)
    ]
    shifted.append(jnp.where(lane == used - 1, roll(tiles[0], used - 1), turned[-1]))
    return shifted


def shift_right(tiles, used, pat):
    lane = pat[0]
    first = lane == 0
    if len(tiles) == 1:
        t = tiles[0]
        last = 64 + used - 1
        return [jnp.where(first, roll(t, -last), roll(t, 1))]
    turned = [roll(t, 1) for t in tiles[:-1]]
    shifted = [jnp.where(first, roll(tiles[-1], -(used - 1)), turned[0])]
    for b in range(1, len(tiles) - 1):
        shifted.append(jnp.where(first, turned[b - 1], turned[b]))
    shifted.append(jnp.where(first, turned[-1], roll(tiles[-1], 1)))
    return shifted


def lat_split(level, tiles, pat):
    main = MAIN[level]
    if level < 3:
        pairs = [split_pair(tiles[2 * b], tiles[2 * b + 1], pat) for b in range(main // 2)]
        pairs.append(split_pair(tiles[main], None, pat))
    else:
        pairs = [split_pair(tiles[0], tiles[1], pat)]
    u = [e + Q * o for e, o in pairs]
    t = shift_left([Q * e - o for e, o in pairs], USED[level] // 2, pat)
    low = [a + R * b for a, b in zip(u, t)]
    high = [b - R * a for a, b in zip(u, t)]
    return low, high


def lat_join(level, low, high, pat):
    main = MAIN[level]
    u = [a - R * b for a, b in zip(low, high)]
    t = shift_right([R * a + b for a, b in zip(low, high)], USED[level] // 2, pat)
    pairs = [(a + Q * b, Q * a - b) for a, b in zip(u, t)]
    if level == 3:
        return join_pair(*pairs[0], pat)
    tiles = []
    for b in range(main // 2):
        tiles += join_pair(*pairs[b], pat)
    if level > 0:
        tiles += join_pair(*pairs[-1], pat, both=False)
    return tiles


def tiles_of(x):
    return [x[:, LANES * b : LANES * (b + 1)] for b in range(x.shape[1] // LANES)]


def wide(tiles):
    return tiles[0] if len(tiles) == 1 else jnp.concatenate(tiles, 1)


def stack(a, b):
    return [jnp.concatenate([x, y], 0) for x, y in zip(a, b)]


def kernel(
    x_hbm, table, band_index, out_hbm,
    xin, xh, oxt, u0, u1, u2, u3, ul,
    c1, c2, c3, g0, g1, g2, b0, b1, b2,
    wh0, wh1, wh2, wh3, wb0, wb1, wb2, wb3, wc,
    tab0, tab1, tab2, tab3, side,
    hl_s, hl_r, hr_s, hr_r, ma_s, ma_r, mb_s, mb_r, mc_s, mc_r, md_s, md_r,
    in_sem, out_sem, send, recv, side_send, side_recv,
):
    chunks = xin.shape[0]
    lon, lat = lax.axis_index("lon"), lax.axis_index("lat")
    lons, lats = lax.axis_size("lon"), lax.axis_size("lat")
    nxt, prv = (lax.rem(lon + 1, lons), lat), (lax.rem(lon + lons - 1, lons), lat)
    right, left = (lon, lat + 1), (lon, lat - 1)
    has_right, has_left = lat < lats - 1, lat > 0

    def load(c, i):
        return pltpu.make_async_copy(
            x_hbm.at[pl.ds(M * c, M), i], xin.at[c, i], in_sem.at[c]
        )

    def store(c, i):
        return pltpu.make_async_copy(
            oxt.at[c, i], out_hbm.at[pl.ds(M * c, M), i], out_sem.at[c]
        )

    def send_to(kind, c, src, dst, to):
        return pltpu.make_async_remote_copy(
            src_ref=src.at[c], dst_ref=dst.at[c],
            send_sem=send.at[kind, c], recv_sem=recv.at[kind, c],
            device_id=to, device_id_type=MESH,
        )

    def begin(c, carry):
        for i in range(LON):
            load(c, i).start()
        return carry

    lax.fori_loop(0, chunks, begin, 0)

    barrier = pltpu.get_barrier_semaphore()
    for to in (nxt, prv):
        pl.semaphore_signal(barrier, inc=1, device_id=to, device_id_type=MESH)

    @pl.when(has_left)
    def _():
        pl.semaphore_signal(barrier, inc=1, device_id=left, device_id_type=MESH)

    @pl.when(has_right)
    def _():
        pl.semaphore_signal(barrier, inc=1, device_id=right, device_id_type=MESH)

    peers = 2 + jnp.where(has_left, 1, 0) + jnp.where(has_right, 1, 0)
    pl.semaphore_wait(barrier, peers)

    last_tile = pl.ds(table.shape[1] - LANES, LANES)

    def side_copy():
        return pltpu.make_async_remote_copy(
            src_ref=table.at[:, last_tile], dst_ref=side,
            send_sem=side_send, recv_sem=side_recv,
            device_id=right, device_id_type=MESH,
        )

    @pl.when(has_right)
    def _():
        side_copy().start()

    def stage_z(c):
        pltpu.make_async_copy(x_hbm.at[pl.ds(M * c, M)], xin.at[c], in_sem.at[c]).wait()
        quarter = lane_ids(M) >> 5
        for k in range(LON // 4):
            to_left = to_right = None
            for n in range(4):
                head = roll(xin[c, 4 * k + n, :, :LANES], HALO * n)
                tail = roll(xin[c, 4 * k + n, :, 7 * LANES :], HALO * (n + 1))
                to_left = head if n == 0 else jnp.where(quarter == n, head, to_left)
                to_right = tail if n == 0 else jnp.where(quarter == n, tail, to_right)
            hr_s[c, k] = to_left
            hl_s[c, k] = to_right

        @pl.when(has_left)
        def _():
            send_to(0, c, hr_s, hr_r, left).start()

        @pl.when(has_right)
        def _():
            send_to(1, c, hl_s, hl_r, right).start()

    def keep(level, p, c, low, high, coarse, bands, highs, wb, wh):
        coarse[c, p] = wide([x[:M] for x in low])
        bands[c, p] = wide([x[M:] for x in low]) * wb[...]
        highs[c, p] = wide(high) * wh[...]

    def field(ref, c, i):
        return tiles_of(ref[c, i])

    def first(e, o):
        return [a + Q * b for a, b in zip(e, o)]

    def second(e, o):
        return [Q * a - b for a, b in zip(e, o)]

    def lon_split(u, t):
        return stack([a + R * b for a, b in zip(u, t)], [b - R * a for a, b in zip(u, t)])

    def lon_join(tiles):
        lo, hi = [x[:M] for x in tiles], [x[M:] for x in tiles]
        return [a - R * b for a, b in zip(lo, hi)], [R * a + b for a, b in zip(lo, hi)]

    def input_field(c, i):
        return tiles_of(xin[c, i]) + [xh[c, i]]

    def stage_a(c):
        @pl.when(has_right)
        def _():
            send_to(0, c, hr_s, hr_r, left).wait_recv()

        @pl.when(has_left)
        def _():
            send_to(1, c, hl_s, hl_r, right).wait_recv()

        pat = patterns(2 * M)
        lane = lane_ids(M)
        in_right = (lane < HALO) & has_right
        in_left = (lane >= HALO) & (lane < 2 * HALO) & has_left
        for i in range(LON):
            k, n = i // 4, i % 4
            r_part = roll(hr_r[c, k], -HALO * n)
            l_part = roll(hl_r[c, k], HALO * (1 - n))
            xh[c, i] = jnp.where(in_right, r_part, jnp.where(in_left, l_part, 0.0))

        x0, x1 = input_field(c, 0), input_field(c, 1)
        t0 = second(x0, x1)
        u = first(x0, x1)
        for p in range(7):
            x0, x1 = input_field(c, 2 * p + 2), input_field(c, 2 * p + 3)
            low, high = lat_split(0, lon_split(u, second(x0, x1)), pat)
            keep(0, p, c, low, high, c1, b0, g0, wb0, wh0)
            u = first(x0, x1)
        u0[c] = wide(u)

        t1 = second(field(c1, c, 0), field(c1, c, 1))
        for p in range(2):
            u = first(field(c1, c, 2 * p), field(c1, c, 2 * p + 1))
            t = second(field(c1, c, 2 * p + 2), field(c1, c, 2 * p + 3))
            low, high = lat_split(1, lon_split(u, t), pat)
            keep(1, p, c, low, high, c2, b1, g1, wb1, wh1)
        t2 = second(field(c2, c, 0), field(c2, c, 1))
        halo = jnp.where(lane < 64, t0[8], jnp.where(lane < 96, roll(t1[4], 64), roll(t2[2], 96)))
        ma_s[c] = wide(t0[:8] + t1[:4] + t2[:2] + [halo])
        send_to(2, c, ma_s, ma_r, prv).start()

    def stage_b(c):
        send_to(2, c, ma_s, ma_r, prv).wait_recv()
        pat = patterns(2 * M)
        got = tiles_of(ma_r[c])
        halo = got[14]
        t0, t1, t2 = got[:8] + [halo], got[8:12] + [roll(halo, -64)], got[12:14] + [roll(halo, -96)]
        low, high = lat_split(0, lon_split(tiles_of(u0[c]), t0), pat)
        keep(0, 7, c, low, high, c1, b0, g0, wb0, wh0)
        for p in (2, 3):
            u = first(field(c1, c, 2 * p), field(c1, c, 2 * p + 1))
            t = second(field(c1, c, 6), field(c1, c, 7)) if p == 2 else t1
            low, high = lat_split(1, lon_split(u, t), pat)
            keep(1, p, c, low, high, c2, b1, g1, wb1, wh1)
        for p in (0, 1):
            u = first(field(c2, c, 2 * p), field(c2, c, 2 * p + 1))
            t = second(field(c2, c, 2), field(c2, c, 3)) if p == 0 else t2
            low, high = lat_split(2, lon_split(u, t), pat)
            keep(2, p, c, low, high, c3, b2, g2, wb2, wh2)
        mb_s[c] = wide(second(field(c3, c, 0), field(c3, c, 1)))
        send_to(3, c, mb_s, mb_r, prv).start()

    def stage_c(c):
        send_to(3, c, mb_s, mb_r, prv).wait_recv()
        pat = patterns(2 * M)
        u = first(field(c3, c, 0), field(c3, c, 1))
        low, high = lat_split(3, lon_split(u, tiles_of(mb_r[c])), pat)
        low = [low[0] * wc[...]]
        high = [high[0] * wh3[...]]
        u, t = lon_join(lat_join(3, low, high, pat))
        u3[c] = wide(u)
        mc_s[c] = wide(t)
        send_to(4, c, mc_s, mc_r, nxt).start()

    def synthesis(level, c, p, coarse, bands, highs, pat):
        return lon_join(
            lat_join(level, stack(field(coarse, c, p), field(bands, c, p)), field(highs, c, p), pat)
        )

    def put(ref, c, p, u, t):
        ref[c, 2 * p] = wide(first(u, t))
        ref[c, 2 * p + 1] = wide(second(u, t))

    def stage_d(c):
        send_to(4, c, mc_s, mc_r, nxt).wait_recv()
        pat = patterns(2 * M)
        lane = lane_ids(M)
        put(c3, c, 0, tiles_of(u3[c]), tiles_of(mc_r[c]))
        u, t_two = synthesis(2, c, 0, c3, b2, g2, pat)
        u2[c] = wide(u)
        u, t2 = synthesis(2, c, 1, c3, b2, g2, pat)
        put(c2, c, 1, u, t_two)
        u, t_one = synthesis(1, c, 2, c2, b1, g1, pat)
        u1[c] = wide(u)
        u, t1 = synthesis(1, c, 3, c2, b1, g1, pat)
        put(c1, c, 3, u, t_one)
        u, t0 = synthesis(0, c, 7, c1, b0, g0, pat)
        ul[c] = wide(u)
        halo = jnp.where(lane < 64, t1[4], roll(t2[2], 64))
        md_s[c] = wide(t0 + t1[:4] + t2[:2] + [halo])
        send_to(5, c, md_s, md_r, nxt).start()

    def stage_e(c):
        send_to(5, c, md_s, md_r, nxt).wait_recv()
        pat = patterns(2 * M)
        got = tiles_of(md_r[c])
        halo = got[14]
        t0, t1, t2 = got[:8], got[8:12] + [halo], got[12:14] + [roll(halo, -64)]
        put(c2, c, 0, tiles_of(u2[c]), t2)
        t = t1
        for p in (0, 1):
            u, t_next = synthesis(1, c, p, c2, b1, g1, pat)
            put(c1, c, p, u, t)
            t = t_next
        put(c1, c, 2, tiles_of(u1[c]), t)
        t = t0
        for p in range(7):
            u, t_next = synthesis(0, c, p, c1, b0, g0, pat)
            put(oxt, c, p, u, t)
            t = t_next
        put(oxt, c, 7, tiles_of(ul[c]), t)
        for i in range(LON):
            store(c, i).start()

    def weights():
        @pl.when(has_right)
        def _():
            side_copy().wait_send()

        @pl.when(has_left)
        def _():
            side_copy().wait_recv()

        pat = patterns(TABLE_ROWS)
        lane, front, even_odd, odd_even, _, _ = pat

        def halved(tiles):
            if len(tiles) == 1:
                return [permute(tiles[0], even_odd)]
            return [
                jnp.where(front, permute(a, even_odd), permute(b, odd_even))
                for a, b in zip(tiles[::2], tiles[1::2])
            ]

        def between(x, lo, hi):
            return jnp.where((lane >= lo) & (lane < hi) & has_left, x, 0.0)

        main, edge = tiles_of(table[...]), side[...]
        tab0[...] = wide(main + [between(roll(edge, 32), 16, 32)]) * H0**4
        main, edge = halved(main), permute(edge, even_odd)
        tab1[...] = wide(main + [between(roll(edge, 80), 8, 16)]) * H0**8
        main, edge = halved(main), permute(edge, even_odd)
        tab2[...] = wide(main + [between(roll(edge, 104), 4, 8)]) * H0**12
        main, edge = halved(main), permute(edge, even_odd)
        tab3[...] = jnp.where(lane < 64, main[0], between(roll(edge, 52), 66, 68)) * H0**16

        def row(tab, i):
            one = tab[pl.ds(band_index[i], 1), :]
            return jnp.broadcast_to(one, (M, one.shape[1]))

        for level, (tab, wh, wb) in enumerate(
            ((tab0, wh0, wb0), (tab1, wh1, wb1), (tab2, wh2, wb2), (tab3, wh3, wb3))
        ):
            wh[:M] = row(tab, 3 * level)
            wh[M:] = row(tab, 3 * level + 2)
            wb[...] = row(tab, 3 * level + 1)
        wc[:M] = row(tab3, 12)
        wc[M:] = wb3[...]

    lax.fori_loop(0, OFFSETS[1], lambda c, carry: (stage_z(c), carry)[1], 0)
    weights()

    def step(s, carry):
        for stage, offset in zip((stage_z, stage_a, stage_b, stage_c, stage_d, stage_e), OFFSETS):
            c = s - offset

            @pl.when((c >= 0) & (c < chunks))
            def _(stage=stage, c=c):
                stage(c)

        return carry

    lax.fori_loop(OFFSETS[1], chunks + OFFSETS[-1], step, 0)

    def finish(c, carry):
        @pl.when(has_left)
        def _():
            send_to(0, c, hr_s, hr_r, left).wait_send()

        @pl.when(has_right)
        def _():
            send_to(1, c, hl_s, hl_r, right).wait_send()

        send_to(2, c, ma_s, ma_r, prv).wait_send()
        send_to(3, c, mb_s, mb_r, prv).wait_send()
        send_to(4, c, mc_s, mc_r, nxt).wait_send()
        send_to(5, c, md_s, md_r, nxt).wait_send()
        pltpu.make_async_copy(oxt.at[c], out_hbm.at[pl.ds(M * c, M)], out_sem.at[c]).wait()
        return carry

    lax.fori_loop(0, chunks, finish, 0)


TABLE_ROWS = 8


def per_device(perturbation, weight_table, band_index):
    members = perturbation.shape[0]
    chunks = members // M
    width = perturbation.shape[2]
    widths = [(m + 1) * LANES for m in MAIN]
    halves = [widths[1], widths[2], widths[3], LANES]

    def vmem(*shape):
        return pltpu.VMEM(shape, F32)

    per = [
        vmem(chunks, LON, M, width), vmem(chunks, LON, M, LANES), vmem(chunks, LON, M, width),
        vmem(chunks, M, widths[0]), vmem(chunks, M, widths[1]), vmem(chunks, M, widths[2]),
        vmem(chunks, M, widths[3]), vmem(chunks, M, width),
        vmem(chunks, 8, M, widths[1]), vmem(chunks, 4, M, widths[2]), vmem(chunks, 2, M, widths[3]),
        vmem(chunks, 8, 2 * M, halves[0]), vmem(chunks, 4, 2 * M, halves[1]),
        vmem(chunks, 2, 2 * M, halves[2]),
        vmem(chunks, 8, M, halves[0]), vmem(chunks, 4, M, halves[1]), vmem(chunks, 2, M, halves[2]),
    ]
    weights = [vmem(2 * M, h) for h in halves] + [vmem(M, h) for h in halves] + [vmem(2 * M, LANES)]
    tables = [vmem(TABLE_ROWS, h) for h in halves] + [vmem(TABLE_ROWS, LANES)]
    messages = [vmem(chunks, LON // 4, M, LANES)] * 4
    messages += [vmem(chunks, M, 15 * LANES)] * 2 + [vmem(chunks, M, 2 * LANES)] * 4
    messages += [vmem(chunks, M, 15 * LANES)] * 2
    dma = pltpu.SemaphoreType.DMA
    return pl.pallas_call(
        kernel,
        out_shape=jax.ShapeDtypeStruct(perturbation.shape, F32),
        in_specs=[
            pl.BlockSpec(memory_space=pl.ANY),
            pl.BlockSpec(memory_space=pltpu.VMEM),
            pl.BlockSpec(memory_space=pltpu.SMEM),
        ],
        out_specs=pl.BlockSpec(memory_space=pl.ANY),
        scratch_shapes=per + weights + tables + messages
        + [dma((chunks,)), dma((chunks,)), dma((6, chunks)), dma((6, chunks)), dma, dma],
        compiler_params=pltpu.CompilerParams(
            collective_id=0, has_side_effects=True, vmem_limit_bytes=60 * 2**20
        ),
    )(perturbation, weight_table, band_index)


def solution(mesh):
    placed = (P(None, "lon", "lat"), P(None, "lat"), P())
    return jax.shard_map(
        per_device, mesh=mesh, in_specs=placed, out_specs=P(None, "lon", "lat"), check_vma=False
    )
```

```python
import math

import jax
import jax.numpy as jnp
import numpy as np
from jax import lax
from jax.experimental import pallas as pl
from jax.experimental.pallas import tpu as pltpu
from jax.sharding import PartitionSpec as P

F32 = jnp.float32
LANES = 128
M = 16
LON = 16
HALO = 32
Q = math.sqrt(3.0)
R = 2.0 - Q
H0 = (1.0 + Q) / (4.0 * math.sqrt(2.0))
MESH = pl.DeviceIdType.MESH
MAIN = (8, 4, 2, 1)
OFFSETS = (0, 2, 4, 6, 8, 10)

GATHER = lax.GatherDimensionNumbers(
    offset_dims=(),
    collapsed_slice_dims=(1,),
    start_index_map=(1,),
    operand_batching_dims=(0,),
    start_indices_batching_dims=(0,),
)


def lane_ids(rows):
    return lax.broadcasted_iota(jnp.int32, (rows, LANES), 1)


def permute(x, index):
    return lax.gather(
        x, index[..., None], GATHER, (1, 1), mode=lax.GatherScatterMode.PROMISE_IN_BOUNDS
    )


def roll(x, by):
    by = by % LANES
    return x if by == 0 else pltpu.roll(x, by, 1)


def patterns(rows):
    lane = lane_ids(rows)
    front = lane < 64
    half = lane & 63
    even_odd = 2 * half + jnp.where(front, 0, 1)
    odd_even = 2 * half + jnp.where(front, 1, 0)
    return lane, front, even_odd, odd_even


def filter_matrices():
    k = np.arange(LANES)
    turned = (k + 1) % LANES
    exact = np.zeros((2 * LANES, 2 * LANES), np.float64)
    exact[2 * k, k], exact[2 * k + 1, k] = 1.0, Q
    exact[2 * turned, LANES + k], exact[2 * turned + 1, LANES + k] = Q, -1.0
    both = []
    for matrix in (exact, exact.T):
        head = matrix.astype(jnp.bfloat16)
        rest = (matrix - head.astype(np.float64)).astype(jnp.bfloat16)
        both.append(np.concatenate([head, head, rest], 0))
    return np.stack(both)


def multiply(blocks, matrix):
    x = jnp.concatenate([wide(pair) for pair in blocks], 0)
    head = x.astype(jnp.bfloat16)
    rest = (x - head.astype(F32)).astype(jnp.bfloat16)
    out = jnp.dot(
        jnp.concatenate([head, rest, head], 1), matrix[...], preferred_element_type=F32
    )
    rows = blocks[0][0].shape[0]
    return [
        (out[rows * b : rows * (b + 1), :LANES], out[rows * b : rows * (b + 1), LANES:])
        for b in range(len(blocks))
    ]


def lat_split(level, tiles, matrix, last):
    if level < 3:
        main, halo = tiles[:-1], tiles[-1]
        blocks = list(zip(main[::2], main[1::2])) + [(halo, halo)]
    else:
        blocks = [tuple(tiles)]
    pairs = multiply(blocks, matrix)
    u, t = [a for a, _ in pairs], [b for _, b in pairs]
    if len(t) > 1:
        t = [jnp.where(last, b, a) for a, b in zip(t, t[1:] + t[:1])]
    low = [a + R * b for a, b in zip(u, t)]
    high = [b - R * a for a, b in zip(u, t)]
    return low, high


def lat_join(level, low, high, matrix, last):
    u = [a - R * b for a, b in zip(low, high)]
    t = [R * a + b for a, b in zip(low, high)]
    if len(t) > 1:
        t = [jnp.where(last, b, a) for a, b in zip(t, t[-1:] + t[:-1])]
    blocks = list(zip(u, t))
    if level == 0:
        blocks = blocks[:-1]
    pairs = multiply(blocks, matrix)
    tiles = [x for pair in pairs for x in pair]
    if level in (1, 2):
        del tiles[-2]
    return tiles


def tiles_of(x):
    return [x[:, LANES * b : LANES * (b + 1)] for b in range(x.shape[1] // LANES)]


def wide(tiles):
    return tiles[0] if len(tiles) == 1 else jnp.concatenate(tiles, 1)


def stack(a, b):
    return [jnp.concatenate([x, y], 0) for x, y in zip(a, b)]


def kernel(
    x_hbm, table, band_index, matrix_hbm, out_hbm,
    xin, xh, oxt, u0, u1, u2, u3, ul,
    c1, c2, c3, g0, g1, g2, b0, b1, b2,
    wh0, wh1, wh2, wh3, wb0, wb1, wb2, wb3, wc,
    tab0, tab1, tab2, tab3, side,
    hl_s, hl_r, hr_s, hr_r, ma_s, ma_r, mb_s, mb_r, mc_s, mc_r, md_s, md_r,
    matrices, in_sem, out_sem, send, recv, side_send, side_recv, matrix_sem,
):
    chunks = xin.shape[0]
    lon, lat = lax.axis_index("lon"), lax.axis_index("lat")
    lons, lats = lax.axis_size("lon"), lax.axis_size("lat")
    nxt, prv = (lax.rem(lon + 1, lons), lat), (lax.rem(lon + lons - 1, lons), lat)
    right, left = (lon, lat + 1), (lon, lat - 1)
    has_right, has_left = lat < lats - 1, lat > 0

    def load(c, i):
        return pltpu.make_async_copy(
            x_hbm.at[pl.ds(M * c, M), i], xin.at[c, i], in_sem.at[c]
        )

    def store(c, i):
        return pltpu.make_async_copy(
            oxt.at[c, i], out_hbm.at[pl.ds(M * c, M), i], out_sem.at[c]
        )

    def send_to(kind, c, src, dst, to):
        return pltpu.make_async_remote_copy(
            src_ref=src.at[c], dst_ref=dst.at[c],
            send_sem=send.at[kind, c], recv_sem=recv.at[kind, c],
            device_id=to, device_id_type=MESH,
        )

    def begin(c, carry):
        for i in range(LON):
            load(c, i).start()
        return carry

    lax.fori_loop(0, chunks, begin, 0)
    matrix_copy = pltpu.make_async_copy(matrix_hbm, matrices, matrix_sem)
    matrix_copy.start()
    forth, back = matrices.at[0], matrices.at[1]

    barrier = pltpu.get_barrier_semaphore()
    for to in (nxt, prv):
        pl.semaphore_signal(barrier, inc=1, device_id=to, device_id_type=MESH)

    @pl.when(has_left)
    def _():
        pl.semaphore_signal(barrier, inc=1, device_id=left, device_id_type=MESH)

    @pl.when(has_right)
    def _():
        pl.semaphore_signal(barrier, inc=1, device_id=right, device_id_type=MESH)

    peers = 2 + jnp.where(has_left, 1, 0) + jnp.where(has_right, 1, 0)
    pl.semaphore_wait(barrier, peers)

    last_tile = pl.ds(table.shape[1] - LANES, LANES)

    def side_copy():
        return pltpu.make_async_remote_copy(
            src_ref=table.at[:, last_tile], dst_ref=side,
            send_sem=side_send, recv_sem=side_recv,
            device_id=right, device_id_type=MESH,
        )

    @pl.when(has_right)
    def _():
        side_copy().start()

    def stage_z(c):
        pltpu.make_async_copy(x_hbm.at[pl.ds(M * c, M)], xin.at[c], in_sem.at[c]).wait()
        quarter = lane_ids(M) >> 5
        for k in range(LON // 4):
            to_left = to_right = None
            for n in range(4):
                head = roll(xin[c, 4 * k + n, :, :LANES], HALO * n)
                tail = roll(xin[c, 4 * k + n, :, 7 * LANES :], HALO * (n + 1))
                to_left = head if n == 0 else jnp.where(quarter == n, head, to_left)
                to_right = tail if n == 0 else jnp.where(quarter == n, tail, to_right)
            hr_s[c, k] = to_left
            hl_s[c, k] = to_right

        @pl.when(has_left)
        def _():
            send_to(0, c, hr_s, hr_r, left).start()

        @pl.when(has_right)
        def _():
            send_to(1, c, hl_s, hl_r, right).start()

    def keep(level, p, c, low, high, coarse, bands, highs, wb, wh):
        coarse[c, p] = wide([x[:M] for x in low])
        bands[c, p] = wide([x[M:] for x in low]) * wb[...]
        highs[c, p] = wide(high) * wh[...]

    def two(level, ps, c, pair, coarse, bands, highs, wb, wh):
        last = lane_ids(4 * M) == LANES - 1
        low, high = lat_split(level, stack(*pair), forth, last)
        for n, p in enumerate(ps):
            rows = slice(2 * M * n, 2 * M * (n + 1))
            keep(level, p, c, [x[rows] for x in low], [x[rows] for x in high],
                 coarse, bands, highs, wb, wh)

    def field(ref, c, i):
        return tiles_of(ref[c, i])

    def first(e, o):
        return [a + Q * b for a, b in zip(e, o)]

    def second(e, o):
        return [Q * a - b for a, b in zip(e, o)]

    def lon_split(u, t):
        return stack([a + R * b for a, b in zip(u, t)], [b - R * a for a, b in zip(u, t)])

    def lon_join(tiles):
        lo, hi = [x[:M] for x in tiles], [x[M:] for x in tiles]
        return [a - R * b for a, b in zip(lo, hi)], [R * a + b for a, b in zip(lo, hi)]

    def input_field(c, i):
        return tiles_of(xin[c, i]) + [xh[c, i]]

    def stage_a(c):
        @pl.when(has_right)
        def _():
            send_to(0, c, hr_s, hr_r, left).wait_recv()

        @pl.when(has_left)
        def _():
            send_to(1, c, hl_s, hl_r, right).wait_recv()

        last = lane_ids(2 * M) == LANES - 1
        lane = lane_ids(M)
        in_front = (lane < HALO) & has_right
        in_right = (lane >= 64) & (lane < 96) & has_right
        in_left = (lane >= 96) & has_left
        for i in range(LON):
            k, n = i // 4, i % 4
            r_part, l_part = hr_r[c, k], hl_r[c, k]
            rest = jnp.where(in_left, roll(l_part, 96 - HALO * n), 0.0)
            rest = jnp.where(in_right, roll(r_part, 64 - HALO * n), rest)
            xh[c, i] = jnp.where(in_front, roll(r_part, -HALO * n), rest)

        x0, x1 = input_field(c, 0), input_field(c, 1)
        t0 = second(x0, x1)
        u = first(x0, x1)
        for p in range(7):
            x0, x1 = input_field(c, 2 * p + 2), input_field(c, 2 * p + 3)
            low, high = lat_split(0, lon_split(u, second(x0, x1)), forth, last)
            keep(0, p, c, low, high, c1, b0, g0, wb0, wh0)
            u = first(x0, x1)
        u0[c] = wide(u)

        t1 = second(field(c1, c, 0), field(c1, c, 1))
        pair = []
        for p in range(2):
            u = first(field(c1, c, 2 * p), field(c1, c, 2 * p + 1))
            t = second(field(c1, c, 2 * p + 2), field(c1, c, 2 * p + 3))
            pair.append(lon_split(u, t))
        two(1, (0, 1), c, pair, c2, b1, g1, wb1, wh1)
        t2 = second(field(c2, c, 0), field(c2, c, 1))
        halo = jnp.where(lane < 32, roll(t2[2], 32), roll(t1[4], 64))
        halo = jnp.where(lane < 64, halo, t0[8])
        ma_s[c] = wide(t0[:8] + t1[:4] + t2[:2] + [halo])
        send_to(2, c, ma_s, ma_r, prv).start()

    def stage_b(c):
        send_to(2, c, ma_s, ma_r, prv).wait_recv()
        last = lane_ids(2 * M) == LANES - 1
        lane = lane_ids(M)
        got = tiles_of(ma_r[c])
        halo = got[14]
        h0 = jnp.where(lane < 32, roll(halo, 64), halo)
        h1 = jnp.where(lane < 64, roll(halo, 96), roll(halo, 64))
        h2 = jnp.where(lane < 64, roll(halo, 112), roll(halo, 96))
        t0, t1, t2 = got[:8] + [h0], got[8:12] + [h1], got[12:14] + [h2]
        low, high = lat_split(0, lon_split(tiles_of(u0[c]), t0), forth, last)
        keep(0, 7, c, low, high, c1, b0, g0, wb0, wh0)
        x0, x1 = field(c1, c, 6), field(c1, c, 7)
        u = first(field(c1, c, 4), field(c1, c, 5))
        pair = [lon_split(u, second(x0, x1)), lon_split(first(x0, x1), t1)]
        two(1, (2, 3), c, pair, c2, b1, g1, wb1, wh1)
        x0, x1 = field(c2, c, 2), field(c2, c, 3)
        u = first(field(c2, c, 0), field(c2, c, 1))
        pair = [lon_split(u, second(x0, x1)), lon_split(first(x0, x1), t2)]
        two(2, (0, 1), c, pair, c3, b2, g2, wb2, wh2)
        mb_s[c] = wide(second(field(c3, c, 0), field(c3, c, 1)))
        send_to(3, c, mb_s, mb_r, prv).start()

    def stage_c(c):
        send_to(3, c, mb_s, mb_r, prv).wait_recv()
        last = lane_ids(2 * M) == LANES - 1
        u = first(field(c3, c, 0), field(c3, c, 1))
        low, high = lat_split(3, lon_split(u, tiles_of(mb_r[c])), forth, last)
        low = [low[0] * wc[...]]
        high = [high[0] * wh3[...]]
        u, t = lon_join(lat_join(3, low, high, back, last))
        u3[c] = wide(u)
        mc_s[c] = wide(t)
        send_to(4, c, mc_s, mc_r, nxt).start()

    def synthesis(level, c, ps, coarse, bands, highs):
        rows = 2 * M
        last = lane_ids(rows * len(ps)) == LANES - 1
        low = [stack(field(coarse, c, p), field(bands, c, p)) for p in ps]
        high = [field(highs, c, p) for p in ps]
        if len(ps) > 1:
            low, high = [stack(*low)], [stack(*high)]
        tiles = lat_join(level, low[0], high[0], back, last)
        return [
            lon_join([x[rows * n : rows * (n + 1)] for x in tiles]) for n in range(len(ps))
        ]

    def put(ref, c, p, u, t):
        ref[c, 2 * p] = wide(first(u, t))
        ref[c, 2 * p + 1] = wide(second(u, t))

    def stage_d(c):
        send_to(4, c, mc_s, mc_r, nxt).wait_recv()
        lane = lane_ids(M)
        put(c3, c, 0, tiles_of(u3[c]), tiles_of(mc_r[c]))
        (u, t_two), (u_two, t2) = synthesis(2, c, (0, 1), c3, b2, g2)
        u2[c] = wide(u)
        put(c2, c, 1, u_two, t_two)
        (u, t_one), (u_one, t1) = synthesis(1, c, (2, 3), c2, b1, g1)
        u1[c] = wide(u)
        put(c1, c, 3, u_one, t_one)
        ((u, t0),) = synthesis(0, c, (7,), c1, b0, g0)
        ul[c] = wide(u)
        halo = jnp.where(lane < 64, roll(t2[2], 64), t1[4])
        md_s[c] = wide(t0 + t1[:4] + t2[:2] + [halo])
        send_to(5, c, md_s, md_r, nxt).start()

    def stage_e(c):
        send_to(5, c, md_s, md_r, nxt).wait_recv()
        got = tiles_of(md_r[c])
        halo = got[14]
        t0, t1, t2 = got[:8], got[8:12] + [halo], got[12:14] + [roll(halo, 64)]
        put(c2, c, 0, tiles_of(u2[c]), t2)
        t = t1
        for p, (u, t_next) in enumerate(synthesis(1, c, (0, 1), c2, b1, g1)):
            put(c1, c, p, u, t)
            t = t_next
        put(c1, c, 2, tiles_of(u1[c]), t)
        t = t0
        for p in range(7):
            ((u, t_next),) = synthesis(0, c, (p,), c1, b0, g0)
            put(oxt, c, p, u, t)
            t = t_next
        put(oxt, c, 7, tiles_of(ul[c]), t)
        for i in range(LON):
            store(c, i).start()

    def weights():
        @pl.when(has_right)
        def _():
            side_copy().wait_send()

        @pl.when(has_left)
        def _():
            side_copy().wait_recv()

        pat = patterns(TABLE_ROWS)
        lane, front, even_odd, odd_even = pat

        def halved(tiles):
            if len(tiles) == 1:
                return [permute(tiles[0], even_odd)]
            return [
                jnp.where(front, permute(a, even_odd), permute(b, odd_even))
                for a, b in zip(tiles[::2], tiles[1::2])
            ]

        def after(x, lo):
            return jnp.where((lane >= lo) & has_left, x, 0.0)

        main, edge = tiles_of(table[...]), side[...]
        tab0[...] = wide(main + [after(edge, 112)]) * H0**4
        main, edge = halved(main), permute(edge, odd_even)
        tab1[...] = wide(main + [after(edge, 120)]) * H0**8
        main, edge = halved(main), permute(edge, odd_even)
        tab2[...] = wide(main + [after(edge, 124)]) * H0**12
        main, edge = halved(main), permute(edge, odd_even)
        tab3[...] = jnp.where(lane < 64, main[0], after(edge, 126)) * H0**16

        def row(tab, i):
            one = tab[pl.ds(band_index[i], 1), :]
            return jnp.broadcast_to(one, (M, one.shape[1]))

        for level, (tab, wh, wb) in enumerate(
            ((tab0, wh0, wb0), (tab1, wh1, wb1), (tab2, wh2, wb2), (tab3, wh3, wb3))
        ):
            wh[:M] = row(tab, 3 * level)
            wh[M:] = row(tab, 3 * level + 2)
            wb[...] = row(tab, 3 * level + 1)
        wc[:M] = row(tab3, 12)
        wc[M:] = wb3[...]

    lax.fori_loop(0, OFFSETS[1], lambda c, carry: (stage_z(c), carry)[1], 0)
    weights()
    matrix_copy.wait()

    def step(s, carry):
        for stage, offset in zip((stage_z, stage_a, stage_b, stage_c, stage_d, stage_e), OFFSETS):
            c = s - offset

            @pl.when((c >= 0) & (c < chunks))
            def _(stage=stage, c=c):
                stage(c)

        return carry

    lax.fori_loop(OFFSETS[1], chunks + OFFSETS[-1], step, 0)

    def finish(c, carry):
        @pl.when(has_left)
        def _():
            send_to(0, c, hr_s, hr_r, left).wait_send()

        @pl.when(has_right)
        def _():
            send_to(1, c, hl_s, hl_r, right).wait_send()

        send_to(2, c, ma_s, ma_r, prv).wait_send()
        send_to(3, c, mb_s, mb_r, prv).wait_send()
        send_to(4, c, mc_s, mc_r, nxt).wait_send()
        send_to(5, c, md_s, md_r, nxt).wait_send()
        pltpu.make_async_copy(oxt.at[c], out_hbm.at[pl.ds(M * c, M)], out_sem.at[c]).wait()
        return carry

    lax.fori_loop(0, chunks, finish, 0)


TABLE_ROWS = 8


def per_device(perturbation, weight_table, band_index):
    members = perturbation.shape[0]
    chunks = members // M
    width = perturbation.shape[2]
    widths = [(m + 1) * LANES for m in MAIN]
    halves = [widths[1], widths[2], widths[3], LANES]

    def vmem(*shape):
        return pltpu.VMEM(shape, F32)

    per = [
        vmem(chunks, LON, M, width), vmem(chunks, LON, M, LANES), vmem(chunks, LON, M, width),
        vmem(chunks, M, widths[0]), vmem(chunks, M, widths[1]), vmem(chunks, M, widths[2]),
        vmem(chunks, M, widths[3]), vmem(chunks, M, width),
        vmem(chunks, 8, M, widths[1]), vmem(chunks, 4, M, widths[2]), vmem(chunks, 2, M, widths[3]),
        vmem(chunks, 8, 2 * M, halves[0]), vmem(chunks, 4, 2 * M, halves[1]),
        vmem(chunks, 2, 2 * M, halves[2]),
        vmem(chunks, 8, M, halves[0]), vmem(chunks, 4, M, halves[1]), vmem(chunks, 2, M, halves[2]),
    ]
    weights = [vmem(2 * M, h) for h in halves] + [vmem(M, h) for h in halves] + [vmem(2 * M, LANES)]
    tables = [vmem(TABLE_ROWS, h) for h in halves] + [vmem(TABLE_ROWS, LANES)]
    messages = [vmem(chunks, LON // 4, M, LANES)] * 4
    messages += [vmem(chunks, M, 15 * LANES)] * 2 + [vmem(chunks, M, 2 * LANES)] * 4
    messages += [vmem(chunks, M, 15 * LANES)] * 2
    dma = pltpu.SemaphoreType.DMA
    return pl.pallas_call(
        kernel,
        out_shape=jax.ShapeDtypeStruct(perturbation.shape, F32),
        in_specs=[
            pl.BlockSpec(memory_space=pl.ANY),
            pl.BlockSpec(memory_space=pltpu.VMEM),
            pl.BlockSpec(memory_space=pltpu.SMEM),
            pl.BlockSpec(memory_space=pl.ANY),
        ],
        out_specs=pl.BlockSpec(memory_space=pl.ANY),
        scratch_shapes=per + weights + tables + messages
        + [pltpu.VMEM((2, 6 * LANES, 2 * LANES), jnp.bfloat16)]
        + [dma((chunks,)), dma((chunks,)), dma((6, chunks)), dma((6, chunks)), dma, dma, dma],
        compiler_params=pltpu.CompilerParams(
            collective_id=0, has_side_effects=True, vmem_limit_bytes=60 * 2**20
        ),
    )(perturbation, weight_table, band_index, jnp.asarray(filter_matrices()))


def solution(mesh):
    placed = (P(None, "lon", "lat"), P(None, "lat"), P())
    return jax.shard_map(
        per_device, mesh=mesh, in_specs=placed, out_specs=P(None, "lon", "lat"), check_vma=False
    )
```

```python
import math

import jax
import jax.numpy as jnp
import numpy as np
from jax import lax
from jax.experimental import pallas as pl
from jax.experimental.pallas import tpu as pltpu
from jax.sharding import PartitionSpec as P

F32 = jnp.float32
LANES = 128
M = 16
LON = 16
HALO = 32
Q = math.sqrt(3.0)
R = 2.0 - Q
H0 = (1.0 + Q) / (4.0 * math.sqrt(2.0))
MESH = pl.DeviceIdType.MESH
MAIN = (8, 4, 2, 1)
OFFSETS = (0, 2, 4, 6, 8, 10)

GATHER = lax.GatherDimensionNumbers(
    offset_dims=(),
    collapsed_slice_dims=(1,),
    start_index_map=(1,),
    operand_batching_dims=(0,),
    start_indices_batching_dims=(0,),
)


def lane_ids(rows):
    return lax.broadcasted_iota(jnp.int32, (rows, LANES), 1)


def permute(x, index):
    return lax.gather(
        x, index[..., None], GATHER, (1, 1), mode=lax.GatherScatterMode.PROMISE_IN_BOUNDS
    )


def roll(x, by):
    by = by % LANES
    return x if by == 0 else pltpu.roll(x, by, 1)


def patterns(rows):
    lane = lane_ids(rows)
    front = lane < 64
    half = lane & 63
    even_odd = 2 * half + jnp.where(front, 0, 1)
    odd_even = 2 * half + jnp.where(front, 1, 0)
    return lane, front, even_odd, odd_even


def filter_matrices():
    k = np.arange(LANES)
    turned = (k + 1) % LANES
    exact = np.zeros((2 * LANES, 2 * LANES), np.float64)
    exact[2 * k, k], exact[2 * k + 1, k] = 1.0, Q
    exact[2 * turned, LANES + k], exact[2 * turned + 1, LANES + k] = Q, -1.0
    both = []
    for matrix in (exact, exact.T):
        head = matrix.astype(jnp.bfloat16)
        rest = (matrix - head.astype(np.float64)).astype(jnp.bfloat16)
        both.append(np.concatenate([head, head, rest], 0))
    return np.stack(both)


def multiply(blocks, matrix):
    x = jnp.concatenate([wide(pair) for pair in blocks], 0)
    head = x.astype(jnp.bfloat16)
    rest = (x - head.astype(F32)).astype(jnp.bfloat16)
    out = jnp.dot(
        jnp.concatenate([head, rest, head], 1), matrix[...], preferred_element_type=F32
    )
    rows = blocks[0][0].shape[0]
    return [
        (out[rows * b : rows * (b + 1), :LANES], out[rows * b : rows * (b + 1), LANES:])
        for b in range(len(blocks))
    ]


def lat_split(level, tiles, matrix, last):
    if level < 3:
        main, halo = tiles[:-1], tiles[-1]
        blocks = list(zip(main[::2], main[1::2])) + [(halo, halo)]
    else:
        blocks = [tuple(tiles)]
    pairs = multiply(blocks, matrix)
    u, t = [a for a, _ in pairs], [b for _, b in pairs]
    if len(t) > 1:
        t = [jnp.where(last, b, a) for a, b in zip(t, t[1:] + t[:1])]
    low = [a + R * b for a, b in zip(u, t)]
    high = [b - R * a for a, b in zip(u, t)]
    return low, high


def lat_join(level, low, high, matrix, last):
    u = [a - R * b for a, b in zip(low, high)]
    t = [R * a + b for a, b in zip(low, high)]
    if len(t) > 1:
        t = [jnp.where(last, b, a) for a, b in zip(t, t[-1:] + t[:-1])]
    blocks = list(zip(u, t))
    if level == 0:
        blocks = blocks[:-1]
    pairs = multiply(blocks, matrix)
    tiles = [x for pair in pairs for x in pair]
    if level in (1, 2):
        del tiles[-2]
    return tiles


def tiles_of(x):
    return [x[:, LANES * b : LANES * (b + 1)] for b in range(x.shape[1] // LANES)]


def wide(tiles):
    return tiles[0] if len(tiles) == 1 else jnp.concatenate(tiles, 1)


def stack(a, b):
    return [jnp.concatenate([x, y], 0) for x, y in zip(a, b)]


def kernel(
    x_hbm, table, band_index, matrix_hbm, out_hbm,
    xin, xh, oxt, u0, u1, u2, u3, ul,
    c1, c2, c3, g0, g1, g2, b0, b1, b2,
    wh0, wh1, wh2, wh3, wb0, wb1, wb2, wb3, wc,
    tab0, tab1, tab2, tab3, side,
    hl_s, hl_r, hr_s, hr_r, mz_s, mz_r, me_s, me_r, ma_s, ma_r, mb_s, mb_r, mc_s, mc_r, md_s, md_r,
    matrices, in_sem, out_sem, send, recv, side_send, side_recv, matrix_sem,
):
    chunks = xin.shape[0]
    lon, lat = lax.axis_index("lon"), lax.axis_index("lat")
    lons, lats = lax.axis_size("lon"), lax.axis_size("lat")
    nxt, prv = (lax.rem(lon + 1, lons), lat), (lax.rem(lon + lons - 1, lons), lat)
    right, left = (lon, lat + 1), (lon, lat - 1)
    has_right, has_left = lat < lats - 1, lat > 0

    def load(c, i):
        return pltpu.make_async_copy(
            x_hbm.at[pl.ds(M * c, M), i], xin.at[c, i], in_sem.at[c]
        )

    def store(c, i):
        return pltpu.make_async_copy(
            oxt.at[c, i], out_hbm.at[pl.ds(M * c, M), i], out_sem.at[c]
        )

    def send_to(kind, c, src, dst, to):
        return pltpu.make_async_remote_copy(
            src_ref=src.at[c], dst_ref=dst.at[c],
            send_sem=send.at[kind, c], recv_sem=recv.at[kind, c],
            device_id=to, device_id_type=MESH,
        )

    def begin(c, carry):
        for i in range(LON):
            load(c, i).start()
        return carry

    lax.fori_loop(0, chunks, begin, 0)
    matrix_copy = pltpu.make_async_copy(matrix_hbm, matrices, matrix_sem)
    matrix_copy.start()
    forth, back = matrices.at[0], matrices.at[1]

    barrier = pltpu.get_barrier_semaphore()
    for to in (nxt, prv):
        pl.semaphore_signal(barrier, inc=1, device_id=to, device_id_type=MESH)

    @pl.when(has_left)
    def _():
        pl.semaphore_signal(barrier, inc=1, device_id=left, device_id_type=MESH)

    @pl.when(has_right)
    def _():
        pl.semaphore_signal(barrier, inc=1, device_id=right, device_id_type=MESH)

    peers = 2 + jnp.where(has_left, 1, 0) + jnp.where(has_right, 1, 0)
    pl.semaphore_wait(barrier, peers)

    last_tile = pl.ds(table.shape[1] - LANES, LANES)

    def side_copy():
        return pltpu.make_async_remote_copy(
            src_ref=table.at[:, last_tile], dst_ref=side,
            send_sem=side_send, recv_sem=side_recv,
            device_id=right, device_id_type=MESH,
        )

    @pl.when(has_right)
    def _():
        side_copy().start()

    def stage_z(c):
        pltpu.make_async_copy(x_hbm.at[pl.ds(M * c, M)], xin.at[c], in_sem.at[c]).wait()
        mz_s[c] = Q * xin[c, 0] - xin[c, 1]
        send_to(6, c, mz_s, mz_r, prv).start()
        quarter = lane_ids(M) >> 5
        for k in range(LON // 4):
            to_left = to_right = None
            for n in range(4):
                head = roll(xin[c, 4 * k + n, :, :LANES], HALO * n)
                tail = roll(xin[c, 4 * k + n, :, 7 * LANES :], HALO * (n + 1))
                to_left = head if n == 0 else jnp.where(quarter == n, head, to_left)
                to_right = tail if n == 0 else jnp.where(quarter == n, tail, to_right)
            hr_s[c, k] = to_left
            hl_s[c, k] = to_right

        @pl.when(has_left)
        def _():
            send_to(0, c, hr_s, hr_r, left).start()

        @pl.when(has_right)
        def _():
            send_to(1, c, hl_s, hl_r, right).start()

    def keep(level, p, c, low, high, coarse, bands, highs, wb, wh):
        coarse[c, p] = wide([x[:M] for x in low])
        bands[c, p] = wide([x[M:] for x in low]) * wb[...]
        highs[c, p] = wide(high) * wh[...]

    def two(level, ps, c, pair, coarse, bands, highs, wb, wh):
        last = lane_ids(4 * M) == LANES - 1
        low, high = lat_split(level, stack(*pair), forth, last)
        for n, p in enumerate(ps):
            rows = slice(2 * M * n, 2 * M * (n + 1))
            keep(level, p, c, [x[rows] for x in low], [x[rows] for x in high],
                 coarse, bands, highs, wb, wh)

    def field(ref, c, i):
        return tiles_of(ref[c, i])

    def first(e, o):
        return [a + Q * b for a, b in zip(e, o)]

    def second(e, o):
        return [Q * a - b for a, b in zip(e, o)]

    def lon_split(u, t):
        return stack([a + R * b for a, b in zip(u, t)], [b - R * a for a, b in zip(u, t)])

    def lon_join(tiles):
        lo, hi = [x[:M] for x in tiles], [x[M:] for x in tiles]
        return [a - R * b for a, b in zip(lo, hi)], [R * a + b for a, b in zip(lo, hi)]

    def input_field(c, i):
        return tiles_of(xin[c, i]) + [xh[c, i]]

    def stage_a(c):
        @pl.when(has_right)
        def _():
            send_to(0, c, hr_s, hr_r, left).wait_recv()

        @pl.when(has_left)
        def _():
            send_to(1, c, hl_s, hl_r, right).wait_recv()

        last = lane_ids(2 * M) == LANES - 1
        lane = lane_ids(M)
        in_front = (lane < HALO) & has_right
        in_right = (lane >= 64) & (lane < 96) & has_right
        in_left = (lane >= 96) & has_left
        for i in range(LON):
            k, n = i // 4, i % 4
            r_part, l_part = hr_r[c, k], hl_r[c, k]
            rest = jnp.where(in_left, roll(l_part, 96 - HALO * n), 0.0)
            rest = jnp.where(in_right, roll(r_part, 64 - HALO * n), rest)
            xh[c, i] = jnp.where(in_front, roll(r_part, -HALO * n), rest)

        x0, x1 = input_field(c, 0), input_field(c, 1)
        t0 = Q * x0[8] - x1[8]
        u = first(x0, x1)
        for p in range(7):
            x0, x1 = input_field(c, 2 * p + 2), input_field(c, 2 * p + 3)
            low, high = lat_split(0, lon_split(u, second(x0, x1)), forth, last)
            keep(0, p, c, low, high, c1, b0, g0, wb0, wh0)
            u = first(x0, x1)
        u0[c] = wide(u)

        t1 = second(field(c1, c, 0), field(c1, c, 1))
        pair = []
        for p in range(2):
            u = first(field(c1, c, 2 * p), field(c1, c, 2 * p + 1))
            t = second(field(c1, c, 2 * p + 2), field(c1, c, 2 * p + 3))
            pair.append(lon_split(u, t))
        two(1, (0, 1), c, pair, c2, b1, g1, wb1, wh1)
        t2 = second(field(c2, c, 0), field(c2, c, 1))
        halo = jnp.where(lane < 32, roll(t2[2], 32), roll(t1[4], 64))
        halo = jnp.where(lane < 64, halo, t0)
        ma_s[c] = wide(t1[:4] + t2[:2] + [halo])
        send_to(2, c, ma_s, ma_r, prv).start()

    def stage_b(c):
        send_to(6, c, mz_s, mz_r, prv).wait_recv()
        send_to(2, c, ma_s, ma_r, prv).wait_recv()
        last = lane_ids(2 * M) == LANES - 1
        lane = lane_ids(M)
        got = tiles_of(ma_r[c])
        halo = got[6]
        h0 = jnp.where(lane < 32, roll(halo, 64), halo)
        h1 = jnp.where(lane < 64, roll(halo, 96), roll(halo, 64))
        h2 = jnp.where(lane < 64, roll(halo, 112), roll(halo, 96))
        t0, t1, t2 = tiles_of(mz_r[c]) + [h0], got[:4] + [h1], got[4:6] + [h2]
        low, high = lat_split(0, lon_split(tiles_of(u0[c]), t0), forth, last)
        keep(0, 7, c, low, high, c1, b0, g0, wb0, wh0)
        x0, x1 = field(c1, c, 6), field(c1, c, 7)
        u = first(field(c1, c, 4), field(c1, c, 5))
        pair = [lon_split(u, second(x0, x1)), lon_split(first(x0, x1), t1)]
        two(1, (2, 3), c, pair, c2, b1, g1, wb1, wh1)
        x0, x1 = field(c2, c, 2), field(c2, c, 3)
        u = first(field(c2, c, 0), field(c2, c, 1))
        pair = [lon_split(u, second(x0, x1)), lon_split(first(x0, x1), t2)]
        two(2, (0, 1), c, pair, c3, b2, g2, wb2, wh2)
        mb_s[c] = wide(second(field(c3, c, 0), field(c3, c, 1)))
        send_to(3, c, mb_s, mb_r, prv).start()

    def stage_c(c):
        send_to(3, c, mb_s, mb_r, prv).wait_recv()
        last = lane_ids(2 * M) == LANES - 1
        u = first(field(c3, c, 0), field(c3, c, 1))
        low, high = lat_split(3, lon_split(u, tiles_of(mb_r[c])), forth, last)
        low = [low[0] * wc[...]]
        high = [high[0] * wh3[...]]
        u, t = lon_join(lat_join(3, low, high, back, last))
        u3[c] = wide(u)
        mc_s[c] = wide(t)
        send_to(4, c, mc_s, mc_r, nxt).start()

    def synthesis(level, c, ps, coarse, bands, highs):
        rows = 2 * M
        last = lane_ids(rows * len(ps)) == LANES - 1
        low = [stack(field(coarse, c, p), field(bands, c, p)) for p in ps]
        high = [field(highs, c, p) for p in ps]
        if len(ps) > 1:
            low, high = [stack(*low)], [stack(*high)]
        tiles = lat_join(level, low[0], high[0], back, last)
        return [
            lon_join([x[rows * n : rows * (n + 1)] for x in tiles]) for n in range(len(ps))
        ]

    def put(ref, c, p, u, t):
        ref[c, 2 * p] = wide(first(u, t))
        ref[c, 2 * p + 1] = wide(second(u, t))

    def stage_d(c):
        send_to(4, c, mc_s, mc_r, nxt).wait_recv()
        lane = lane_ids(M)
        put(c3, c, 0, tiles_of(u3[c]), tiles_of(mc_r[c]))
        (u, t_two), (u_two, t2) = synthesis(2, c, (0, 1), c3, b2, g2)
        u2[c] = wide(u)
        put(c2, c, 1, u_two, t_two)
        (u, t_one), (u_one, t1) = synthesis(1, c, (2, 3), c2, b1, g1)
        u1[c] = wide(u)
        put(c1, c, 3, u_one, t_one)
        halo = jnp.where(lane < 64, roll(t2[2], 64), t1[4])
        md_s[c] = wide(t1[:4] + t2[:2] + [halo])
        send_to(5, c, md_s, md_r, nxt).start()
        ((u, t0),) = synthesis(0, c, (7,), c1, b0, g0)
        ul[c] = wide(u)
        me_s[c] = wide(t0)
        send_to(7, c, me_s, me_r, nxt).start()

    def stage_e(c):
        send_to(5, c, md_s, md_r, nxt).wait_recv()
        got = tiles_of(md_r[c])
        halo = got[6]
        t1, t2 = got[:4] + [halo], got[4:6] + [roll(halo, 64)]
        put(c2, c, 0, tiles_of(u2[c]), t2)
        t = t1
        for p, (u, t_next) in enumerate(synthesis(1, c, (0, 1), c2, b1, g1)):
            put(c1, c, p, u, t)
            t = t_next
        put(c1, c, 2, tiles_of(u1[c]), t)
        send_to(7, c, me_s, me_r, nxt).wait_recv()
        t = tiles_of(me_r[c])
        for p in range(7):
            ((u, t_next),) = synthesis(0, c, (p,), c1, b0, g0)
            put(oxt, c, p, u, t)
            t = t_next
        put(oxt, c, 7, tiles_of(ul[c]), t)
        for i in range(LON):
            store(c, i).start()

    def weights():
        @pl.when(has_right)
        def _():
            side_copy().wait_send()

        @pl.when(has_left)
        def _():
            side_copy().wait_recv()

        pat = patterns(TABLE_ROWS)
        lane, front, even_odd, odd_even = pat

        def halved(tiles):
            if len(tiles) == 1:
                return [permute(tiles[0], even_odd)]
            return [
                jnp.where(front, permute(a, even_odd), permute(b, odd_even))
                for a, b in zip(tiles[::2], tiles[1::2])
            ]

        def after(x, lo):
            return jnp.where((lane >= lo) & has_left, x, 0.0)

        main, edge = tiles_of(table[...]), side[...]
        tab0[...] = wide(main + [after(edge, 112)]) * H0**4
        main, edge = halved(main), permute(edge, odd_even)
        tab1[...] = wide(main + [after(edge, 120)]) * H0**8
        main, edge = halved(main), permute(edge, odd_even)
        tab2[...] = wide(main + [after(edge, 124)]) * H0**12
        main, edge = halved(main), permute(edge, odd_even)
        tab3[...] = jnp.where(lane < 64, main[0], after(edge, 126)) * H0**16

        def row(tab, i):
            one = tab[pl.ds(band_index[i], 1), :]
            return jnp.broadcast_to(one, (M, one.shape[1]))

        for level, (tab, wh, wb) in enumerate(
            ((tab0, wh0, wb0), (tab1, wh1, wb1), (tab2, wh2, wb2), (tab3, wh3, wb3))
        ):
            wh[:M] = row(tab, 3 * level)
            wh[M:] = row(tab, 3 * level + 2)
            wb[...] = row(tab, 3 * level + 1)
        wc[:M] = row(tab3, 12)
        wc[M:] = wb3[...]

    lax.fori_loop(0, OFFSETS[1], lambda c, carry: (stage_z(c), carry)[1], 0)
    weights()
    matrix_copy.wait()

    def step(s, carry):
        for stage, offset in zip((stage_z, stage_a, stage_b, stage_c, stage_d, stage_e), OFFSETS):
            c = s - offset

            @pl.when((c >= 0) & (c < chunks))
            def _(stage=stage, c=c):
                stage(c)

        return carry

    lax.fori_loop(OFFSETS[1], chunks + OFFSETS[-1], step, 0)

    def finish(c, carry):
        @pl.when(has_left)
        def _():
            send_to(0, c, hr_s, hr_r, left).wait_send()

        @pl.when(has_right)
        def _():
            send_to(1, c, hl_s, hl_r, right).wait_send()

        send_to(2, c, ma_s, ma_r, prv).wait_send()
        send_to(3, c, mb_s, mb_r, prv).wait_send()
        send_to(4, c, mc_s, mc_r, nxt).wait_send()
        send_to(5, c, md_s, md_r, nxt).wait_send()
        send_to(6, c, mz_s, mz_r, prv).wait_send()
        send_to(7, c, me_s, me_r, nxt).wait_send()
        pltpu.make_async_copy(oxt.at[c], out_hbm.at[pl.ds(M * c, M)], out_sem.at[c]).wait()
        return carry

    lax.fori_loop(0, chunks, finish, 0)


TABLE_ROWS = 8


def hand_over(y, out, held, in_sem, out_sem):
    chunks = held.shape[0]
    size = y.shape[0] // chunks

    def load(c):
        return pltpu.make_async_copy(y.at[pl.ds(size * c, size)], held.at[c], in_sem.at[c])

    def store(c):
        return pltpu.make_async_copy(held.at[c], out.at[pl.ds(size * c, size)], out_sem.at[c])

    for c in range(chunks):
        load(c).start()
    for c in range(chunks):
        load(c).wait()
        store(c).start()
    for c in range(chunks):
        store(c).wait()


def per_device(perturbation, weight_table, band_index):
    members = perturbation.shape[0]
    chunks = members // M
    width = perturbation.shape[2]
    widths = [(m + 1) * LANES for m in MAIN]
    halves = [widths[1], widths[2], widths[3], LANES]

    def vmem(*shape):
        return pltpu.VMEM(shape, F32)

    per = [
        vmem(chunks, LON, M, width), vmem(chunks, LON, M, LANES), vmem(chunks, LON, M, width),
        vmem(chunks, M, widths[0]), vmem(chunks, M, widths[1]), vmem(chunks, M, widths[2]),
        vmem(chunks, M, widths[3]), vmem(chunks, M, width),
        vmem(chunks, 8, M, widths[1]), vmem(chunks, 4, M, widths[2]), vmem(chunks, 2, M, widths[3]),
        vmem(chunks, 8, 2 * M, halves[0]), vmem(chunks, 4, 2 * M, halves[1]),
        vmem(chunks, 2, 2 * M, halves[2]),
        vmem(chunks, 8, M, halves[0]), vmem(chunks, 4, M, halves[1]), vmem(chunks, 2, M, halves[2]),
    ]
    weights = [vmem(2 * M, h) for h in halves] + [vmem(M, h) for h in halves] + [vmem(2 * M, LANES)]
    tables = [vmem(TABLE_ROWS, h) for h in halves] + [vmem(TABLE_ROWS, LANES)]
    messages = [vmem(chunks, LON // 4, M, LANES)] * 4 + [vmem(chunks, M, width)] * 4
    messages += [vmem(chunks, M, 7 * LANES)] * 2 + [vmem(chunks, M, 2 * LANES)] * 4
    messages += [vmem(chunks, M, 7 * LANES)] * 2
    dma = pltpu.SemaphoreType.DMA
    result = pl.pallas_call(
        kernel,
        out_shape=jax.ShapeDtypeStruct(perturbation.shape, F32),
        in_specs=[
            pl.BlockSpec(memory_space=pl.ANY),
            pl.BlockSpec(memory_space=pltpu.VMEM),
            pl.BlockSpec(memory_space=pltpu.SMEM),
            pl.BlockSpec(memory_space=pl.ANY),
        ],
        out_specs=pl.BlockSpec(memory_space=pl.ANY),
        scratch_shapes=per + weights + tables + messages
        + [pltpu.VMEM((2, 6 * LANES, 2 * LANES), jnp.bfloat16)]
        + [dma((chunks,)), dma((chunks,)), dma((8, chunks)), dma((8, chunks)), dma, dma, dma],
        compiler_params=pltpu.CompilerParams(
            collective_id=0, has_side_effects=True, vmem_limit_bytes=60 * 2**20
        ),
    )(perturbation, weight_table, band_index, jnp.asarray(filter_matrices()))
    return pl.pallas_call(
        hand_over,
        out_shape=jax.ShapeDtypeStruct(perturbation.shape, F32),
        in_specs=[pl.BlockSpec(memory_space=pl.ANY)],
        out_specs=pl.BlockSpec(memory_space=pl.ANY),
        scratch_shapes=[vmem(10, members // 10, LON, width), dma((10,)), dma((10,))],
        compiler_params=pltpu.CompilerParams(vmem_limit_bytes=60 * 2**20),
    )(result)


def solution(mesh):
    placed = (P(None, "lon", "lat"), P(None, "lat"), P())
    return jax.shard_map(
        per_device, mesh=mesh, in_specs=placed, out_specs=P(None, "lon", "lat"), check_vma=False
    )
```
